32 devices in a mesh: dp: 8 (over z, x), blk: 4 (over y, core).
Axes of the slice: x: 2, y: 2, z: 4, core: 2. Of those that a mesh axis runs over, the one named last changes fastest.
Arguments:
- queries: bfloat16 [8, 512, 2048], P('dp', 'blk'), may hold values from -6 to 6
- keys: bfloat16 [8, 512, 512], P('dp', 'blk'), may hold values from -6 to 6
- values: bfloat16 [8, 512, 512], P('dp', 'blk'), may hold values from -6 to 6
- out_grad: bfloat16 [8, 512, 2048], P('dp', 'blk'), may hold values from -6 to 6
- layer_input: bfloat16 [8, 512, 4096], P('dp', 'blk'), may hold values from -6 to 6
- lengths: int32 [8, 3], P('dp'), may hold values from 32 to 448, as said below
Outputs:
- query_grad: bfloat16 [8, 512, 2048], P('dp', 'blk')
- key_grad: bfloat16 [8, 512, 512], P('dp', 'blk')
- value_grad: bfloat16 [8, 512, 512], P('dp', 'blk')
- weight_grad: float32 [4096, 1024], P(('dp', 'blk'))
The draws below stay inside these ranges and needn't reach their ends.
Inputs may be any that keep to these rules, and one draw needn't show every extreme that they name: `lengths`: each row sums to 512; the chosen and rejected counts lie between 32 and 96.
All inputs are finite; a program needn't handle non-finite values.
Results may differ from the reference program's by a relative error of at most 0.023.
Values may be sent and summed in bfloat16 or wider, within the bound.
A program may use at most 128 MiB of HBM per device.

```python
import math
import jax
import jax.numpy as jnp
from jax import lax

D = 4096
H = 16
KV = 4
HEAD = 128
TOK_DEV = 128
SEQ_LEN = 512
SEQS = 8
N_BLK = 4


def draw_queries(key, part):
    own_key = jax.random.fold_in(key, 1)
    normal_key = jax.random.fold_in(own_key, 0)
    values_drawn = jax.random.normal(normal_key, (SEQS, SEQ_LEN, H * HEAD), jnp.float32)
    return jnp.clip(values_drawn, -6.0, 6.0).astype(jnp.bfloat16)


def draw_keys(key, part):
    own_key = jax.random.fold_in(key, 2)
    normal_key = jax.random.fold_in(own_key, 0)
    values_drawn = jax.random.normal(normal_key, (SEQS, SEQ_LEN, KV * HEAD), jnp.float32)
    return jnp.clip(values_drawn, -6.0, 6.0).astype(jnp.bfloat16)


def draw_lengths(key, part):
    first_key, second_key = jax.random.split(jax.random.fold_in(key, 5))
    lowest = SEQ_LEN // 16
    highest = 3 * SEQ_LEN // 16 + 1
    chosen_len = jax.random.randint(first_key, (SEQS,), lowest, highest)
    rejected_len = jax.random.randint(second_key, (SEQS,), lowest, highest)
    prompt_len = SEQ_LEN - chosen_len - rejected_len
    return jnp.stack([prompt_len, chosen_len, rejected_len], axis=1).astype(jnp.int32)


def block_levels(key, dims, pieces, least, top_value):
    def one(axis_at, parts):
        draws = jax.random.uniform(jax.random.fold_in(jax.random.fold_in(key, 6), axis_at), (parts,), jnp.float32, least / len(pieces), top_value / len(pieces))
        return jnp.repeat(jnp.exp(draws), dims[axis_at] // parts).reshape((-1,) + (1,) * (len(dims) - axis_at - 1))

    loudness = one(*pieces[0])
    for cut in pieces[1:]:
        loudness = loudness * one(*cut)
    return loudness


def normal_values(rng, shape, deviation, bound, cuts=(), kind=jnp.bfloat16):
    level = block_levels(rng, shape, cuts, -0.22, 0.18) if cuts else 1.0
    entries = jax.random.normal(rng, shape, jnp.float32) * deviation * level
    return jnp.minimum(jnp.maximum(entries, -bound), bound).astype(kind)


def setup_inputs(seed: int = 0) -> dict:
    key_list = jax.random.split(jax.random.key(seed), 7)
    return {
        "queries": draw_queries(jax.random.fold_in(key_list[6], 71), 0),
        "keys": draw_keys(jax.random.fold_in(key_list[6], 71), 0),
        "values": normal_values(key_list[2], (SEQS, SEQ_LEN, KV * HEAD), 1.0, 6.0, ((0, 8), (1, 4))),
        "out_grad": normal_values(key_list[3], (SEQS, SEQ_LEN, H * HEAD), 1.0, 6.0, ((0, 8), (1, 4))),
        "layer_input": normal_values(key_list[4], (SEQS, SEQ_LEN, D), 1.0, 6.0, ((0, 8), (1, 4))),
        "lengths": draw_lengths(jax.random.fold_in(key_list[6], 71), 0),
    }


rope_base = 500000.0
masked_fill = -1e+30

def stored_positions(stored_rows, shard_rows, shard_count):
    half_rows = shard_rows // 2
    block_number = stored_rows // half_rows
    holder = block_number // 2
    upper_half = block_number % 2
    position_block = jnp.where(upper_half == 1, 2 * shard_count - 1 - holder, holder)
    return (position_block * half_rows + stored_rows % half_rows).astype(jnp.int32)

def allowed_pairs(query_pos, key_pos, prompt_len, chosen_len):
    causal = key_pos[None, :] <= query_pos[:, None]
    reject_start = prompt_len + chosen_len
    query_rejected = query_pos >= reject_start
    key_chosen = jnp.logical_and(key_pos >= prompt_len, key_pos < reject_start)
    return jnp.logical_and(causal, jnp.logical_not(jnp.logical_and(query_rejected[:, None], key_chosen[None, :])))

def rope_inverse(grad_sum, positions):
    half_dim = HEAD // 2
    frequency = jnp.exp(-(2.0 * jnp.arange(half_dim, dtype=jnp.float32) / HEAD) * math.log(rope_base))
    angles = positions.astype(jnp.float32)[:, None] * frequency[None, :]
    cosine = jnp.concatenate([jnp.cos(angles), jnp.cos(angles)], axis=-1)[:, None, :]
    sine = jnp.concatenate([jnp.sin(angles), jnp.sin(angles)], axis=-1)[:, None, :]
    grad_heads = grad_sum.reshape(grad_sum.shape[0], -1, HEAD)
    rotated = jnp.concatenate([-grad_heads[..., half_dim:], grad_heads[..., :half_dim]], axis=-1)
    return (grad_heads * cosine - rotated * sine).reshape(grad_sum.shape[0], -1).astype(jnp.bfloat16)

def one_sequence(operands):
    queries, keys, values, out_grad, lengths = operands
    seq_len = queries.shape[0]
    group_heads = H // KV
    scale = 1.0 / math.sqrt(HEAD)
    positions = stored_positions(jnp.arange(seq_len, dtype=jnp.int32), TOK_DEV, N_BLK)
    allowed = allowed_pairs(positions, positions, lengths[0], lengths[1])
    query_heads = queries.reshape(seq_len, KV, group_heads, HEAD).transpose(1, 2, 0, 3).astype(jnp.float32)
    grad_heads = out_grad.reshape(seq_len, KV, group_heads, HEAD).transpose(1, 2, 0, 3).astype(jnp.float32)
    key_heads = keys.reshape(seq_len, KV, HEAD).transpose(1, 0, 2).astype(jnp.float32)
    value_heads = values.reshape(seq_len, KV, HEAD).transpose(1, 0, 2).astype(jnp.float32)

    def one_group(group_operands):
        group_query, group_key, group_value, group_grad = group_operands
        scores = scale * jnp.einsum('hqe,ke->hqk', group_query, group_key)
        row_max = lax.optimization_barrier(jnp.max(jnp.where(allowed[None], scores, masked_fill), axis=-1))
        weights = jnp.where(allowed[None], jnp.exp(scores - row_max[..., None]), 0.0)
        row_sum = lax.optimization_barrier(jnp.sum(weights, axis=-1))
        attn_out = jnp.einsum('hqk,ke->hqe', weights, group_value, precision=lax.Precision.HIGHEST) / row_sum[..., None]
        log_total = row_max + jnp.log(row_sum)
        delta = lax.optimization_barrier(jnp.sum(group_grad * attn_out, axis=-1))
        probs = jnp.where(allowed[None], jnp.exp(scores - log_total[..., None]), 0.0)
        prob_half = probs.astype(jnp.bfloat16)
        prob_grad = jnp.einsum('hqe,ke->hqk', group_grad, group_value)
        score_grad = (scale * probs * (prob_grad - delta[..., None])).astype(jnp.bfloat16)
        query_grad = jnp.einsum('hqk,ke->hqe', score_grad.astype(jnp.float32), group_key)
        score_shards = score_grad.astype(jnp.float32).reshape(group_heads, N_BLK, TOK_DEV, seq_len)
        prob_shards = prob_half.astype(jnp.float32).reshape(group_heads, N_BLK, TOK_DEV, seq_len)
        query_shards = group_query.reshape(group_heads, N_BLK, TOK_DEV, HEAD)
        grad_shards = group_grad.reshape(group_heads, N_BLK, TOK_DEV, HEAD)
        key_parts = lax.optimization_barrier(jnp.einsum('hdqk,hdqe->dke', score_shards, query_shards).astype(jnp.bfloat16))
        value_parts = lax.optimization_barrier(jnp.einsum('hdqk,hdqe->dke', prob_shards, grad_shards).astype(jnp.bfloat16))
        key_sum = lax.optimization_barrier(jnp.sum(key_parts.astype(jnp.float32), axis=0))
        value_sum = lax.optimization_barrier(jnp.sum(value_parts.astype(jnp.float32), axis=0))
        return (query_grad, key_sum, value_sum)
    query_grad, key_sum, value_sum = lax.map(one_group, (query_heads, key_heads, value_heads, grad_heads))
    query_grad = query_grad.transpose(2, 0, 1, 3).reshape(seq_len, H * HEAD).astype(jnp.bfloat16)
    key_sum = key_sum.transpose(1, 0, 2).reshape(seq_len, KV * HEAD)
    value_sum = value_sum.transpose(1, 0, 2).reshape(seq_len, KV * HEAD)
    key_pre = rope_inverse(key_sum, positions)
    value_grad = value_sum.astype(jnp.bfloat16)
    grad_cols = jnp.concatenate([key_pre, value_grad], axis=1)
    return (query_grad, key_sum.astype(jnp.bfloat16), value_grad, grad_cols)

def reference(queries, keys, values, out_grad, layer_input, lengths):
    query_grad, key_grad, value_grad, grad_cols = lax.map(one_sequence, (queries, keys, values, out_grad, lengths))
    features = layer_input.shape[2]
    weight_grad = jnp.dot(layer_input.reshape(-1, features).T, grad_cols.reshape(-1, grad_cols.shape[2]), preferred_element_type=jnp.float32)
    return (query_grad, key_grad, value_grad, weight_grad)
```

```python
import functools
import math

import jax
import jax.numpy as jnp
import numpy as np
from jax import lax
from jax.experimental import pallas as pl
from jax.experimental.pallas import tpu as pltpu
from jax.sharding import PartitionSpec as P

HEAD = 128


rope_base = 500000.0
masked_fill = -1e30


def stored_positions(stored_rows, shard_rows, shard_count):
    half_rows = shard_rows // 2
    block_number = stored_rows // half_rows
    holder = block_number // 2
    upper_half = block_number % 2
    position_block = jnp.where(upper_half == 1, 2 * shard_count - 1 - holder, holder)
    return (position_block * half_rows + stored_rows % half_rows).astype(jnp.int32)


def allowed_pairs(query_pos, key_pos, prompt_len, chosen_len):
    causal = key_pos[None, :] <= query_pos[:, None]
    reject_start = prompt_len + chosen_len
    query_rejected = query_pos >= reject_start
    key_chosen = jnp.logical_and(key_pos >= prompt_len, key_pos < reject_start)
    return jnp.logical_and(
        causal, jnp.logical_not(jnp.logical_and(query_rejected[:, None], key_chosen[None, :]))
    )


def block_length(total_rows):
    chosen_size = 1
    for candidate in range(1, min(total_rows, 512) + 1):
        if total_rows % candidate == 0:
            chosen_size = candidate
    return chosen_size


def over_blocks(running, pieces, first_row, block_fn):
    total_rows = pieces[0].shape[0]
    block_rows = block_length(total_rows)

    def one_turn(turn_index, current):
        block_start = turn_index * block_rows
        block_parts = tuple(
            (lax.dynamic_slice_in_dim(member, block_start, block_rows, 0) for member in pieces)
        )
        return block_fn(current, block_parts, first_row + block_start)

    return lax.fori_loop(0, total_rows // block_rows, one_turn, running)


def body(queries, keys, values, out_grad, layer_input, lengths):
    shard_count = lax.axis_size("blk")
    shard_index = lax.axis_index("blk")
    shard_rows = queries.shape[1]
    kv_heads = keys.shape[2] // HEAD
    group_heads = queries.shape[2] // keys.shape[2]
    seq_len = shard_rows * shard_count
    query_count = group_heads * shard_rows
    scale = 1.0 / math.sqrt(HEAD)
    prompt_len = lengths[0, 0]
    chosen_len = lengths[0, 1]
    own_rows = shard_index * shard_rows + jnp.arange(shard_rows, dtype=jnp.int32)
    own_pos = stored_positions(own_rows, shard_rows, shard_count)
    query_pos = jnp.tile(own_pos, group_heads)
    query_rows = (
        queries[0]
        .reshape(shard_rows, kv_heads, group_heads, HEAD)
        .transpose(1, 2, 0, 3)
        .reshape(kv_heads, query_count, HEAD)
    )
    grad_rows = (
        out_grad[0]
        .reshape(shard_rows, kv_heads, group_heads, HEAD)
        .transpose(1, 2, 0, 3)
        .reshape(kv_heads, query_count, HEAD)
    )

    def block_allowed(first_row, count_rows):
        key_pos = stored_positions(
            first_row + jnp.arange(count_rows, dtype=jnp.int32), shard_rows, shard_count
        )
        return allowed_pairs(query_pos, key_pos, prompt_len, chosen_len)

    def forward_block(running, block_parts, first_row):
        key_block, value_block = block_parts
        count_rows = key_block.shape[0]
        allowed = block_allowed(first_row, count_rows)
        run_max, run_sum, run_acc = running
        key_heads = key_block.reshape(count_rows, kv_heads, HEAD)
        value_heads = value_block.reshape(count_rows, kv_heads, HEAD).astype(jnp.float32)
        scores = scale * jnp.einsum(
            "gqe,kge->gqk", query_rows, key_heads, preferred_element_type=jnp.float32
        )
        new_max = jnp.maximum(
            run_max, jnp.max(jnp.where(allowed[None], scores, masked_fill), axis=-1)
        )
        weights = jnp.where(allowed[None], jnp.exp(scores - new_max[..., None]), 0.0)
        factor = jnp.exp(run_max - new_max)
        new_sum = run_sum * factor + jnp.sum(weights, axis=-1)
        new_acc = run_acc * factor[..., None] + jnp.einsum(
            "gqk,kge->gqe", weights, value_heads, precision=lax.Precision.HIGHEST
        )
        return (new_max, new_sum, new_acc)

    start_forward = (
        jnp.full((kv_heads, query_count), masked_fill, jnp.float32),
        jnp.zeros((kv_heads, query_count), jnp.float32),
        jnp.zeros((kv_heads, query_count, HEAD), jnp.float32),
    )
    run_max, run_sum, run_acc = over_blocks(
        start_forward,
        (
            lax.all_gather(keys[0], "blk", axis=0, tiled=True),
            lax.all_gather(values[0], "blk", axis=0, tiled=True),
        ),
        jnp.int32(0),
        forward_block,
    )
    attn_out = run_acc / run_sum[..., None]
    log_total = run_max + jnp.log(run_sum)
    delta = jnp.sum(grad_rows.astype(jnp.float32) * attn_out, axis=-1)

    def backward_block(running, block_parts, first_row):
        key_block, value_block = block_parts
        count_rows = key_block.shape[0]
        allowed = block_allowed(first_row, count_rows)
        query_acc, key_acc, value_acc = running
        key_heads = key_block.reshape(count_rows, kv_heads, HEAD)
        value_heads = value_block.reshape(count_rows, kv_heads, HEAD)
        scores = scale * jnp.einsum(
            "gqe,kge->gqk", query_rows, key_heads, preferred_element_type=jnp.float32
        )
        probs = jnp.where(allowed[None], jnp.exp(scores - log_total[..., None]), 0.0)
        prob_half = probs.astype(jnp.bfloat16)
        prob_grad = jnp.einsum(
            "gqe,kge->gqk", grad_rows, value_heads, preferred_element_type=jnp.float32
        )
        score_grad = (scale * probs * (prob_grad - delta[..., None])).astype(jnp.bfloat16)
        query_acc = query_acc + jnp.einsum(
            "gqk,kge->gqe", score_grad, key_heads, preferred_element_type=jnp.float32
        )
        key_term = jnp.einsum(
            "gqk,gqe->kge", score_grad, query_rows, preferred_element_type=jnp.float32
        ).reshape(count_rows, kv_heads * HEAD)
        value_term = jnp.einsum(
            "gqk,gqe->kge", prob_half, grad_rows, preferred_element_type=jnp.float32
        ).reshape(count_rows, kv_heads * HEAD)
        key_acc = lax.dynamic_update_slice_in_dim(
            key_acc,
            lax.dynamic_slice_in_dim(key_acc, first_row, count_rows, 0) + key_term,
            first_row,
            0,
        )
        value_acc = lax.dynamic_update_slice_in_dim(
            value_acc,
            lax.dynamic_slice_in_dim(value_acc, first_row, count_rows, 0) + value_term,
            first_row,
            0,
        )
        return (query_acc, key_acc, value_acc)

    start_backward = (
        jnp.zeros((kv_heads, query_count, HEAD), jnp.float32),
        jnp.zeros((seq_len, kv_heads * HEAD), jnp.float32),
        jnp.zeros((seq_len, kv_heads * HEAD), jnp.float32),
    )
    query_acc, key_acc, value_acc = over_blocks(
        start_backward,
        (
            lax.all_gather(keys[0], "blk", axis=0, tiled=True),
            lax.all_gather(values[0], "blk", axis=0, tiled=True),
        ),
        jnp.int32(0),
        backward_block,
    )
    key_sum, value_sum = (
        lax.psum_scatter(
            key_acc.astype(jnp.bfloat16), "blk", scatter_dimension=0, tiled=True
        ).astype(jnp.float32),
        lax.psum_scatter(
            value_acc.astype(jnp.bfloat16), "blk", scatter_dimension=0, tiled=True
        ).astype(jnp.float32),
    )
    query_grad = (
        query_acc.reshape(kv_heads, group_heads, shard_rows, HEAD)
        .transpose(2, 0, 1, 3)
        .reshape(shard_rows, kv_heads * group_heads * HEAD)
        .astype(jnp.bfloat16)
    )
    key_out = key_sum.astype(jnp.bfloat16)
    value_out = value_sum.astype(jnp.bfloat16)
    half_dim = HEAD // 2
    frequency = jnp.exp(
        -(2.0 * jnp.arange(half_dim, dtype=jnp.float32) / HEAD) * math.log(rope_base)
    )
    angles = own_pos.astype(jnp.float32)[:, None] * frequency[None, :]
    cosine = jnp.concatenate([jnp.cos(angles), jnp.cos(angles)], axis=-1)[:, None, :]
    sine = jnp.concatenate([jnp.sin(angles), jnp.sin(angles)], axis=-1)[:, None, :]
    grad_heads = key_sum.reshape(shard_rows, kv_heads, HEAD)
    rotated = jnp.concatenate([-grad_heads[..., half_dim:], grad_heads[..., :half_dim]], axis=-1)
    key_pre = (
        (grad_heads * cosine - rotated * sine)
        .reshape(shard_rows, kv_heads * HEAD)
        .astype(jnp.bfloat16)
    )
    grad_cols = jnp.concatenate([key_pre, value_out], axis=1)
    input_rows = layer_input[0]
    features = layer_input.shape[2]
    replica_count = lax.axis_size("dp")
    feature_share = features // (replica_count * shard_count)
    grouped_input = input_rows.reshape(shard_rows, replica_count, shard_count * feature_share)
    sequence_input = lax.all_to_all(grouped_input, "blk", split_axis=2, concat_axis=0, tiled=True)
    sequence_weight = jnp.einsum(
        "tif,tc->ifc",
        sequence_input,
        lax.all_gather(grad_cols, "blk", axis=0, tiled=True),
        preferred_element_type=jnp.float32,
    )
    weight_grad = (
        lax.psum_scatter(
            sequence_weight.astype(jnp.bfloat16), "dp", scatter_dimension=0, tiled=True
        )
        .astype(jnp.float32)
        .reshape(feature_share, grad_cols.shape[1])
    )
    return (query_grad[None], key_out[None], value_out[None], weight_grad)


def flipped(coordinate, bit):
    return 1 - coordinate if bit else coordinate


def fused_kernel(
    sizes, len_ref, q_ref, k_ref, v_ref, o_ref, x_ref, cos_ref, sin_ref,
    qg_ref, kg_ref, vg_ref, w_ref,
    qbuf, obuf, kbuf, vbuf, dqbuf, acc, part, precv, kgbuf, gbuf, xin, xt, wbuf, zrecv,
    local_sem, send_sem, recv_sem,
):
    rows, local_heads, group, shards, depth = sizes
    seq = rows * shards
    half = rows // 2
    kv_heads = 2 * local_heads
    kv_cols = local_heads * HEAD
    head_cols = group * HEAD
    q_cols = local_heads * head_cols
    scale = 1.0 / math.sqrt(HEAD)
    dp, b = lax.axis_index("dp"), lax.axis_index("blk")
    z, x = dp // 2, dp % 2
    y, c = b // 2, b % 2

    def peer(rx, ry, rc):
        px, py, pc = flipped(x, rx), flipped(y, ry), flipped(c, rc)
        return px, py, pc

    def target(rx, ry, rc):
        px, py, pc = peer(rx, ry, rc)
        return (2 * z + px, 2 * py + pc)

    counts = {"local": 0, "remote": 0}
    pending = []

    def local(src, dst):
        at = counts["local"]
        counts["local"] += 1
        copy = pltpu.make_async_copy(src, dst, local_sem.at[at])
        copy.start()
        return copy

    def remote(src, dst, landing, device):
        at = counts["remote"]
        counts["remote"] += 1
        copy = pltpu.make_async_remote_copy(
            src_ref=src, dst_ref=dst, send_sem=send_sem.at[at], recv_sem=recv_sem.at[at],
            device_id=device, device_id_type=pl.DeviceIdType.MESH,
        )
        copy.start()
        pending.append(copy)
        return pltpu.make_async_remote_copy(
            src_ref=src, dst_ref=landing, send_sem=send_sem.at[at], recv_sem=recv_sem.at[at],
            device_id=device, device_id_type=pl.DeviceIdType.MESH,
        )

    def cols(start, count):
        return pl.ds(pl.multiple_of(start, HEAD), count)

    def rows_of(shard):
        return pl.ds(pl.multiple_of(shard * rows, rows), rows)

    flips = [(rx, ry, rc) for rx in (0, 1) for ry in (0, 1) for rc in (0, 1)]
    barrier = pltpu.get_barrier_semaphore()
    for flip in flips[1:]:
        pl.semaphore_signal(
            barrier, inc=1, device_id=target(*flip), device_id_type=pl.DeviceIdType.MESH
        )
    for offset in range(1, depth):
        pl.semaphore_signal(
            barrier, inc=1, device_id=(2 * ((z + offset) % depth) + x, b),
            device_id_type=pl.DeviceIdType.MESH,
        )
    own = [
        local(k_ref.at[:, cols(c * kv_cols, kv_cols)], kbuf.at[b]),
        local(v_ref.at[:, cols(c * kv_cols, kv_cols)], vbuf.at[b]),
        local(q_ref.at[:, cols(c * q_cols, q_cols)], qbuf.at[c]),
        local(o_ref.at[:, cols(c * q_cols, q_cols)], obuf.at[c]),
    ]
    group_at = x * shards + b

    def features(zz, px, py, pc):
        return cols(((2 * zz + px) * shards + 2 * py + pc) * HEAD, HEAD)

    own_x = [
        local(x_ref.at[:, features(zz, x, y, c)], xin.at[zz, group_at]) for zz in range(depth)
    ]
    pl.semaphore_wait(barrier, 7 + depth - 1)

    first = []
    for flip in ((0, 1, 0), (0, 1, 1), (0, 0, 1)):
        _, py, pc = peer(*flip)
        other = 2 * py + pc
        for ref, buf in ((k_ref, kbuf), (v_ref, vbuf)):
            first.append(
                remote(ref.at[:, cols(pc * kv_cols, kv_cols)], buf.at[b], buf.at[other], target(*flip))
            )
    for ref, buf in ((q_ref, qbuf), (o_ref, obuf)):
        first.append(
            remote(
                ref.at[:, cols((1 - c) * q_cols, q_cols)], buf.at[c], buf.at[1 - c], target(0, 0, 1)
            )
        )
    for copy in own:
        copy.wait()
    for copy in first:
        copy.wait_recv()
    exchange = []
    for flip in flips[1:]:
        px, py, pc = peer(*flip)
        other = px * shards + 2 * py + pc
        for zz in range(depth):
            exchange.append(
                remote(
                    x_ref.at[:, features(zz, px, py, pc)], xin.at[zz, group_at],
                    xin.at[zz, other], target(*flip),
                )
            )

    prompt_len, chosen_len = len_ref[0, 0], len_ref[0, 1]
    reject_start = prompt_len + chosen_len
    key_row = lax.broadcasted_iota(jnp.int32, (seq, 1), 0)
    key_pos = stored_positions(key_row, rows, shards)
    chosen = jnp.logical_and(key_pos >= prompt_len, key_pos < reject_start)
    key_end = jnp.where(chosen, reject_start, 2 * seq)
    lane_row = lax.broadcasted_iota(jnp.int32, (1, head_cols), 1) % rows
    part_copies, out_copies = [], []
    for i in range(local_heads):
        keys = kbuf[:, :, i * HEAD : (i + 1) * HEAD].reshape(seq, HEAD)
        values = vbuf[:, :, i * HEAD : (i + 1) * HEAD].reshape(seq, HEAD)
        acc[...] = jnp.zeros_like(acc)

        def unit(a, carry):
            shard = 2 * y + a
            low = shard * half
            high = (2 * shards - 1 - shard) * half
            query_pos = jnp.where(lane_row >= half, high - half + lane_row, low + lane_row)
            starts = [(i * group + h) * HEAD for h in range(group)]
            queries = jnp.concatenate([qbuf[a, :, s : s + HEAD] for s in starts], axis=0)
            grads = jnp.concatenate([obuf[a, :, s : s + HEAD] for s in starts], axis=0)
            last = (((1,), (1,)), ((), ()))
            first_dims = (((0,), (0,)), ((), ()))
            scores = lax.dot_general(keys, queries, last, preferred_element_type=jnp.float32)
            prob_grad = lax.dot_general(values, grads, last, preferred_element_type=jnp.float32)
            allowed = jnp.logical_and(key_pos <= query_pos, query_pos < key_end)
            scores = jnp.where(allowed, scores, masked_fill)
            top = jnp.max(scores, axis=0, keepdims=True)
            weights = jnp.exp((scores - top) * scale)
            inverse = 1.0 / jnp.sum(weights, axis=0, keepdims=True)
            delta = jnp.sum(weights * prob_grad, axis=0, keepdims=True) * inverse
            probs = (weights * inverse).astype(jnp.bfloat16)
            score_grad = (weights * (prob_grad - delta) * (scale * inverse)).astype(jnp.bfloat16)
            acc[:, :HEAD] += jnp.dot(score_grad, queries, preferred_element_type=jnp.float32)
            acc[:, HEAD:] += jnp.dot(probs, grads, preferred_element_type=jnp.float32)
            query_grad = lax.dot_general(
                score_grad, keys, first_dims, preferred_element_type=jnp.float32
            ).astype(jnp.bfloat16)
            for h in range(group):
                dqbuf[i, a, :, h * HEAD : (h + 1) * HEAD] = query_grad[h * rows : (h + 1) * rows]
            return carry

        lax.fori_loop(0, 2, unit, 0)
        part[i] = acc[...].astype(jnp.bfloat16)
        part_copies.append(remote(part.at[i], precv.at[i], precv.at[i], target(0, 1, 0)))
        own_cols = cols((c * local_heads + i) * head_cols, head_cols)
        other_cols = cols(((1 - c) * local_heads + i) * head_cols, head_cols)
        out_copies.append(
            remote(
                dqbuf.at[i, 1 - c], qg_ref.at[:, own_cols], qg_ref.at[:, other_cols], target(0, 0, 1)
            )
        )
        own.append(local(dqbuf.at[i, c], qg_ref.at[:, own_cols]))

    for copy in own_x:
        copy.wait()
    for copy in exchange:
        copy.wait_recv()
    for zz in range(depth):
        for at in range(2 * shards):
            xt[zz, :, at * rows : (at + 1) * rows] = xin[zz, at].T

    sibling = 2 * y + 1 - c
    to_x, to_sibling = [], []
    for i in range(local_heads):
        part_copies[i].wait_recv()
        total = part[i].astype(jnp.float32) + precv[i].astype(jnp.float32)
        key_sum, value_sum = total[:, :HEAD], total[:, HEAD:]
        kgbuf[i] = key_sum.astype(jnp.bfloat16)
        g, other_g = c * local_heads + i, (1 - c) * local_heads + i
        turned = pltpu.roll(key_sum, HEAD // 2, 1)
        gbuf[g, x, :, :HEAD] = (key_sum * cos_ref[...] + turned * sin_ref[...]).astype(jnp.bfloat16)
        gbuf[g, x, :, HEAD:] = value_sum.astype(jnp.bfloat16)
        to_x.append(remote(gbuf.at[g, x], gbuf.at[g, x], gbuf.at[g, 1 - x], target(1, 0, 0)))
        to_sibling.append(
            remote(gbuf.at[g, x], gbuf.at[g, x], gbuf.at[other_g, x], target(0, 0, 1))
        )
        own_cols, other_cols = cols(g * HEAD, HEAD), cols(other_g * HEAD, HEAD)
        for buf, out in (
            (kgbuf.at[i], kg_ref),
            (gbuf.at[g, x, :, HEAD : 2 * HEAD], vg_ref),
        ):
            own.append(local(buf.at[rows_of(b), :], out.at[:, own_cols]))
            out_copies.append(
                remote(
                    buf.at[rows_of(sibling), :], out.at[:, own_cols], out.at[:, other_cols],
                    target(0, 0, 1),
                )
            )

    scattered = []
    for i in range(local_heads):
        g, other_g = c * local_heads + i, (1 - c) * local_heads + i
        to_x[i].wait_recv()
        relayed = remote(
            gbuf.at[g, 1 - x], gbuf.at[g, 1 - x], gbuf.at[other_g, 1 - x], target(0, 0, 1)
        )
        to_sibling[i].wait_recv()
        relayed.wait_recv()
        for j in range(2):
            grad_cols = gbuf[j * local_heads + i].reshape(2 * seq, 2 * HEAD)
            for zz in range(depth):
                wbuf[i, zz, :, j * 2 * HEAD : (j + 1) * 2 * HEAD] = jnp.dot(
                    xt[zz], grad_cols, preferred_element_type=jnp.float32
                ).astype(jnp.bfloat16)
        for offset in range(1, depth):
            far = (z + offset) % depth
            scattered.append(
                remote(
                    wbuf.at[i, far], zrecv.at[i, offset - 1], zrecv.at[i, offset - 1],
                    (2 * far + x, b),
                )
            )

    for i in range(local_heads):
        total = wbuf[i, z].astype(jnp.float32)
        for offset in range(1, depth):
            scattered[i * (depth - 1) + offset - 1].wait_recv()
            total = total + zrecv[i, offset - 1].astype(jnp.float32)
        for j in range(2):
            g = j * local_heads + i
            for kind in range(2):
                at = kind * kv_heads * HEAD + g * HEAD
                piece = (2 * j + kind) * HEAD
                w_ref[:, at : at + HEAD] = total[:, piece : piece + HEAD]
    for copy in own[4:]:
        copy.wait()
    for copy in out_copies:
        copy.wait_recv()
    for copy in pending:
        copy.wait_send()


def fused_body(queries, keys, values, out_grad, layer_input, lengths):
    shards = lax.axis_size("blk")
    depth = lax.axis_size("dp") // 2
    rows = queries.shape[1]
    kv_heads = keys.shape[2] // HEAD
    local_heads = kv_heads // 2
    group = queries.shape[2] // keys.shape[2]
    seq = rows * shards
    half_dim = HEAD // 2
    stored = np.arange(seq)
    block = stored // (rows // 2)
    holder = block // 2
    block = np.where(block % 2 == 1, 2 * shards - 1 - holder, holder)
    positions = (block * (rows // 2) + stored % (rows // 2)).astype(np.float32)
    frequency = np.exp(
        -(np.float32(2.0) * np.arange(half_dim, dtype=np.float32) / np.float32(HEAD))
        * np.float32(math.log(rope_base))
    ).astype(np.float32)
    angles = positions[:, None] * frequency[None, :]
    cosine = np.concatenate([np.cos(angles), np.cos(angles)], axis=1).astype(np.float32)
    sine = np.concatenate([np.sin(angles), -np.sin(angles)], axis=1).astype(np.float32)
    vmem = pl.BlockSpec(memory_space=pltpu.VMEM)
    anywhere = pl.BlockSpec(memory_space=pl.ANY)
    half = jnp.bfloat16
    q_cols = local_heads * group * HEAD
    kv_cols = local_heads * HEAD
    remote_count = 8 + 7 * depth + 2 * local_heads + 4 * local_heads + local_heads
    remote_count += local_heads * (depth - 1)
    local_count = 4 + depth + 3 * local_heads
    features = layer_input.shape[2] // (2 * depth * shards)
    assert features == HEAD
    outs = pl.pallas_call(
        functools.partial(fused_kernel, (rows, local_heads, group, shards, depth)),
        out_shape=(
            jax.ShapeDtypeStruct(queries.shape[1:], half),
            jax.ShapeDtypeStruct(keys.shape[1:], half),
            jax.ShapeDtypeStruct(values.shape[1:], half),
            jax.ShapeDtypeStruct((features, 2 * kv_heads * HEAD), jnp.float32),
        ),
        in_specs=[pl.BlockSpec(memory_space=pltpu.SMEM)] + [anywhere] * 5 + [vmem] * 2,
        out_specs=(vmem,) * 4,
        scratch_shapes=[
            pltpu.VMEM((2, rows, q_cols), half),
            pltpu.VMEM((2, rows, q_cols), half),
            pltpu.VMEM((shards, rows, kv_cols), half),
            pltpu.VMEM((shards, rows, kv_cols), half),
            pltpu.VMEM((local_heads, 2, rows, group * HEAD), half),
            pltpu.VMEM((seq, 2 * HEAD), jnp.float32),
            pltpu.VMEM((local_heads, seq, 2 * HEAD), half),
            pltpu.VMEM((local_heads, seq, 2 * HEAD), half),
            pltpu.VMEM((local_heads, seq, HEAD), half),
            pltpu.VMEM((kv_heads, 2, seq, 2 * HEAD), half),
            pltpu.VMEM((depth, 2 * shards, rows, features), half),
            pltpu.VMEM((depth, features, 2 * seq), half),
            pltpu.VMEM((local_heads, depth, features, 4 * HEAD), half),
            pltpu.VMEM((local_heads, depth - 1, features, 4 * HEAD), half),
            pltpu.SemaphoreType.DMA((local_count,)),
            pltpu.SemaphoreType.DMA((remote_count,)),
            pltpu.SemaphoreType.DMA((remote_count,)),
        ],
        compiler_params=pltpu.CompilerParams(
            collective_id=0, has_side_effects=True, vmem_limit_bytes=56 * 1024 * 1024
        ),
    )(
        lengths, queries[0], keys[0], values[0], out_grad[0], layer_input[0],
        jnp.asarray(cosine), jnp.asarray(sine),
    )
    query_grad, key_grad, value_grad, weight_grad = outs
    return (query_grad[None], key_grad[None], value_grad[None], weight_grad)


def chosen_body(queries, keys, values, out_grad, layer_input, lengths):
    shards, replicas = lax.axis_size("blk"), lax.axis_size("dp")
    paired = shards == 2 * 2 and replicas % 2 == 0 and replicas > 2
    kv_heads = keys.shape[2] // HEAD
    even = kv_heads % 2 == 0 and queries.shape[1] % HEAD == 0
    if paired and even and layer_input.shape[2] == replicas * shards * HEAD:
        return fused_body(queries, keys, values, out_grad, layer_input, lengths)
    return body(queries, keys, values, out_grad, layer_input, lengths)


def solution(mesh):
    placed = (
        P("dp", "blk", None),
        P("dp", "blk", None),
        P("dp", "blk", None),
        P("dp", "blk", None),
        P("dp", "blk", None),
        P("dp", None),
    )
    return jax.shard_map(
        chosen_body,
        mesh=mesh,
        in_specs=placed,
        out_specs=(
            P("dp", "blk", None),
            P("dp", "blk", None),
            P("dp", "blk", None),
            P(("dp", "blk"), None),
        ),
        check_vma=False,
    )
```

```python
import functools
import math

import jax
import jax.numpy as jnp
import numpy as np
from jax import lax
from jax.experimental import pallas as pl
from jax.experimental.pallas import tpu as pltpu
from jax.sharding import PartitionSpec as P

HEAD = 128


rope_base = 500000.0
masked_fill = -1e30


def stored_positions(stored_rows, shard_rows, shard_count):
    half_rows = shard_rows // 2
    block_number = stored_rows // half_rows
    holder = block_number // 2
    upper_half = block_number % 2
    position_block = jnp.where(upper_half == 1, 2 * shard_count - 1 - holder, holder)
    return (position_block * half_rows + stored_rows % half_rows).astype(jnp.int32)


def allowed_pairs(query_pos, key_pos, prompt_len, chosen_len):
    causal = key_pos[None, :] <= query_pos[:, None]
    reject_start = prompt_len + chosen_len
    query_rejected = query_pos >= reject_start
    key_chosen = jnp.logical_and(key_pos >= prompt_len, key_pos < reject_start)
    return jnp.logical_and(
        causal, jnp.logical_not(jnp.logical_and(query_rejected[:, None], key_chosen[None, :]))
    )


def block_length(total_rows):
    chosen_size = 1
    for candidate in range(1, min(total_rows, 512) + 1):
        if total_rows % candidate == 0:
            chosen_size = candidate
    return chosen_size


def over_blocks(running, pieces, first_row, block_fn):
    total_rows = pieces[0].shape[0]
    block_rows = block_length(total_rows)

    def one_turn(turn_index, current):
        block_start = turn_index * block_rows
        block_parts = tuple(
            (lax.dynamic_slice_in_dim(member, block_start, block_rows, 0) for member in pieces)
        )
        return block_fn(current, block_parts, first_row + block_start)

    return lax.fori_loop(0, total_rows // block_rows, one_turn, running)


def body(queries, keys, values, out_grad, layer_input, lengths):
    shard_count = lax.axis_size("blk")
    shard_index = lax.axis_index("blk")
    shard_rows = queries.shape[1]
    kv_heads = keys.shape[2] // HEAD
    group_heads = queries.shape[2] // keys.shape[2]
    seq_len = shard_rows * shard_count
    query_count = group_heads * shard_rows
    scale = 1.0 / math.sqrt(HEAD)
    prompt_len = lengths[0, 0]
    chosen_len = lengths[0, 1]
    own_rows = shard_index * shard_rows + jnp.arange(shard_rows, dtype=jnp.int32)
    own_pos = stored_positions(own_rows, shard_rows, shard_count)
    query_pos = jnp.tile(own_pos, group_heads)
    query_rows = (
        queries[0]
        .reshape(shard_rows, kv_heads, group_heads, HEAD)
        .transpose(1, 2, 0, 3)
        .reshape(kv_heads, query_count, HEAD)
    )
    grad_rows = (
        out_grad[0]
        .reshape(shard_rows, kv_heads, group_heads, HEAD)
        .transpose(1, 2, 0, 3)
        .reshape(kv_heads, query_count, HEAD)
    )

    def block_allowed(first_row, count_rows):
        key_pos = stored_positions(
            first_row + jnp.arange(count_rows, dtype=jnp.int32), shard_rows, shard_count
        )
        return allowed_pairs(query_pos, key_pos, prompt_len, chosen_len)

    def forward_block(running, block_parts, first_row):
        key_block, value_block = block_parts
        count_rows = key_block.shape[0]
        allowed = block_allowed(first_row, count_rows)
        run_max, run_sum, run_acc = running
        key_heads = key_block.reshape(count_rows, kv_heads, HEAD)
        value_heads = value_block.reshape(count_rows, kv_heads, HEAD).astype(jnp.float32)
        scores = scale * jnp.einsum(
            "gqe,kge->gqk", query_rows, key_heads, preferred_element_type=jnp.float32
        )
        new_max = jnp.maximum(
            run_max, jnp.max(jnp.where(allowed[None], scores, masked_fill), axis=-1)
        )
        weights = jnp.where(allowed[None], jnp.exp(scores - new_max[..., None]), 0.0)
        factor = jnp.exp(run_max - new_max)
        new_sum = run_sum * factor + jnp.sum(weights, axis=-1)
        new_acc = run_acc * factor[..., None] + jnp.einsum(
            "gqk,kge->gqe", weights, value_heads, precision=lax.Precision.HIGHEST
        )
        return (new_max, new_sum, new_acc)

    start_forward = (
        jnp.full((kv_heads, query_count), masked_fill, jnp.float32),
        jnp.zeros((kv_heads, query_count), jnp.float32),
        jnp.zeros((kv_heads, query_count, HEAD), jnp.float32),
    )
    run_max, run_sum, run_acc = over_blocks(
        start_forward,
        (
            lax.all_gather(keys[0], "blk", axis=0, tiled=True),
            lax.all_gather(values[0], "blk", axis=0, tiled=True),
        ),
        jnp.int32(0),
        forward_block,
    )
    attn_out = run_acc / run_sum[..., None]
    log_total = run_max + jnp.log(run_sum)
    delta = jnp.sum(grad_rows.astype(jnp.float32) * attn_out, axis=-1)

    def backward_block(running, block_parts, first_row):
        key_block, value_block = block_parts
        count_rows = key_block.shape[0]
        allowed = block_allowed(first_row, count_rows)
        query_acc, key_acc, value_acc = running
        key_heads = key_block.reshape(count_rows, kv_heads, HEAD)
        value_heads = value_block.reshape(count_rows, kv_heads, HEAD)
        scores = scale * jnp.einsum(
            "gqe,kge->gqk", query_rows, key_heads, preferred_element_type=jnp.float32
        )
        probs = jnp.where(allowed[None], jnp.exp(scores - log_total[..., None]), 0.0)
        prob_half = probs.astype(jnp.bfloat16)
        prob_grad = jnp.einsum(
            "gqe,kge->gqk", grad_rows, value_heads, preferred_element_type=jnp.float32
        )
        score_grad = (scale * probs * (prob_grad - delta[..., None])).astype(jnp.bfloat16)
        query_acc = query_acc + jnp.einsum(
            "gqk,kge->gqe", score_grad, key_heads, preferred_element_type=jnp.float32
        )
        key_term = jnp.einsum(
            "gqk,gqe->kge", score_grad, query_rows, preferred_element_type=jnp.float32
        ).reshape(count_rows, kv_heads * HEAD)
        value_term = jnp.einsum(
            "gqk,gqe->kge", prob_half, grad_rows, preferred_element_type=jnp.float32
        ).reshape(count_rows, kv_heads * HEAD)
        key_acc = lax.dynamic_update_slice_in_dim(
            key_acc,
            lax.dynamic_slice_in_dim(key_acc, first_row, count_rows, 0) + key_term,
            first_row,
            0,
        )
        value_acc = lax.dynamic_update_slice_in_dim(
            value_acc,
            lax.dynamic_slice_in_dim(value_acc, first_row, count_rows, 0) + value_term,
            first_row,
            0,
        )
        return (query_acc, key_acc, value_acc)

    start_backward = (
        jnp.zeros((kv_heads, query_count, HEAD), jnp.float32),
        jnp.zeros((seq_len, kv_heads * HEAD), jnp.float32),
        jnp.zeros((seq_len, kv_heads * HEAD), jnp.float32),
    )
    query_acc, key_acc, value_acc = over_blocks(
        start_backward,
        (
            lax.all_gather(keys[0], "blk", axis=0, tiled=True),
            lax.all_gather(values[0], "blk", axis=0, tiled=True),
        ),
        jnp.int32(0),
        backward_block,
    )
    key_sum, value_sum = (
        lax.psum_scatter(
            key_acc.astype(jnp.bfloat16), "blk", scatter_dimension=0, tiled=True
        ).astype(jnp.float32),
        lax.psum_scatter(
            value_acc.astype(jnp.bfloat16), "blk", scatter_dimension=0, tiled=True
        ).astype(jnp.float32),
    )
    query_grad = (
        query_acc.reshape(kv_heads, group_heads, shard_rows, HEAD)
        .transpose(2, 0, 1, 3)
        .reshape(shard_rows, kv_heads * group_heads * HEAD)
        .astype(jnp.bfloat16)
    )
    key_out = key_sum.astype(jnp.bfloat16)
    value_out = value_sum.astype(jnp.bfloat16)
    half_dim = HEAD // 2
    frequency = jnp.exp(
        -(2.0 * jnp.arange(half_dim, dtype=jnp.float32) / HEAD) * math.log(rope_base)
    )
    angles = own_pos.astype(jnp.float32)[:, None] * frequency[None, :]
    cosine = jnp.concatenate([jnp.cos(angles), jnp.cos(angles)], axis=-1)[:, None, :]
    sine = jnp.concatenate([jnp.sin(angles), jnp.sin(angles)], axis=-1)[:, None, :]
    grad_heads = key_sum.reshape(shard_rows, kv_heads, HEAD)
    rotated = jnp.concatenate([-grad_heads[..., half_dim:], grad_heads[..., :half_dim]], axis=-1)
    key_pre = (
        (grad_heads * cosine - rotated * sine)
        .reshape(shard_rows, kv_heads * HEAD)
        .astype(jnp.bfloat16)
    )
    grad_cols = jnp.concatenate([key_pre, value_out], axis=1)
    input_rows = layer_input[0]
    features = layer_input.shape[2]
    replica_count = lax.axis_size("dp")
    feature_share = features // (replica_count * shard_count)
    grouped_input = input_rows.reshape(shard_rows, replica_count, shard_count * feature_share)
    sequence_input = lax.all_to_all(grouped_input, "blk", split_axis=2, concat_axis=0, tiled=True)
    sequence_weight = jnp.einsum(
        "tif,tc->ifc",
        sequence_input,
        lax.all_gather(grad_cols, "blk", axis=0, tiled=True),
        preferred_element_type=jnp.float32,
    )
    weight_grad = (
        lax.psum_scatter(
            sequence_weight.astype(jnp.bfloat16), "dp", scatter_dimension=0, tiled=True
        )
        .astype(jnp.float32)
        .reshape(feature_share, grad_cols.shape[1])
    )
    return (query_grad[None], key_out[None], value_out[None], weight_grad)


def flipped(coordinate, bit):
    return 1 - coordinate if bit else coordinate


def fused_kernel(
    sizes, len_ref, q_ref, k_ref, v_ref, o_ref, x_ref, cos_ref, sin_ref,
    qg_ref, kg_ref, vg_ref, w_ref,
    qbuf, obuf, kbuf, vbuf, dqbuf, acc, part, precv, kgbuf, gbuf, xin, xt, wbuf, zrecv, wown,
    local_sem, send_sem, recv_sem,
):
    rows, local_heads, group, shards, depth = sizes
    seq = rows * shards
    half = rows // 2
    kv_heads = 2 * local_heads
    head_cols = group * HEAD
    scale = 1.0 / math.sqrt(HEAD)
    dp, b = lax.axis_index("dp"), lax.axis_index("blk")
    z, x = dp // 2, dp % 2
    y, c = b // 2, b % 2

    def peer(rx, ry, rc):
        px, py, pc = flipped(x, rx), flipped(y, ry), flipped(c, rc)
        return px, py, pc

    def target(rx, ry, rc):
        px, py, pc = peer(rx, ry, rc)
        return (2 * z + px, 2 * py + pc)

    counts = {"local": 0, "remote": 0}
    pending = []

    def local(src, dst):
        at = counts["local"]
        counts["local"] += 1
        copy = pltpu.make_async_copy(src, dst, local_sem.at[at])
        copy.start()
        return copy

    def remote(src, dst, landing, device):
        at = counts["remote"]
        counts["remote"] += 1
        copy = pltpu.make_async_remote_copy(
            src_ref=src, dst_ref=dst, send_sem=send_sem.at[at], recv_sem=recv_sem.at[at],
            device_id=device, device_id_type=pl.DeviceIdType.MESH,
        )
        copy.start()
        pending.append(copy)
        return pltpu.make_async_remote_copy(
            src_ref=src, dst_ref=landing, send_sem=send_sem.at[at], recv_sem=recv_sem.at[at],
            device_id=device, device_id_type=pl.DeviceIdType.MESH,
        )

    def cols(start, count):
        return pl.ds(pl.multiple_of(start, HEAD), count)

    def rows_of(shard):
        return pl.ds(pl.multiple_of(shard * rows, rows), rows)

    flips = [(rx, ry, rc) for rx in (0, 1) for ry in (0, 1) for rc in (0, 1)]
    barrier = pltpu.get_barrier_semaphore()
    for flip in flips[1:]:
        pl.semaphore_signal(
            barrier, inc=1, device_id=target(*flip), device_id_type=pl.DeviceIdType.MESH
        )
    moves = [(1, 1), (0, 1), (1, 0), (0, 0)]

    def moved(outer, inner):
        return 2 * flipped(z // 2, outer) + flipped(z % 2, inner)

    for move in moves[:-1]:
        pl.semaphore_signal(
            barrier, inc=1, device_id=(2 * moved(*move) + x, b),
            device_id_type=pl.DeviceIdType.MESH,
        )
    own = []
    for i in range(local_heads):
        at = c * local_heads + i
        own.append(local(k_ref.at[:, cols(at * HEAD, HEAD)], kbuf.at[i, b]))
        own.append(local(v_ref.at[:, cols(at * HEAD, HEAD)], vbuf.at[i, b]))
        own.append(local(q_ref.at[:, cols(at * head_cols, head_cols)], qbuf.at[i, c]))
        own.append(local(o_ref.at[:, cols(at * head_cols, head_cols)], obuf.at[i, c]))
    own_count = len(own)
    group_at = x * shards + b

    def features(zz, px, py, pc):
        return cols(((2 * zz + px) * shards + 2 * py + pc) * HEAD, HEAD)

    own_x = [
        local(x_ref.at[:, features(zz, x, y, c)], xin.at[zz, group_at]) for zz in range(depth)
    ]
    pl.semaphore_wait(barrier, len(flips) - 1 + len(moves) - 1)

    first = []
    for i in range(local_heads):
        arriving = []
        for flip in ((0, 1, 0), (0, 1, 1), (0, 0, 1)):
            _, py, pc = peer(*flip)
            other = 2 * py + pc
            columns = cols((pc * local_heads + i) * HEAD, HEAD)
            for ref, buf in ((k_ref, kbuf), (v_ref, vbuf)):
                arriving.append(
                    remote(ref.at[:, columns], buf.at[i, b], buf.at[i, other], target(*flip))
                )
        columns = cols(((1 - c) * local_heads + i) * head_cols, head_cols)
        for ref, buf in ((q_ref, qbuf), (o_ref, obuf)):
            arriving.append(
                remote(ref.at[:, columns], buf.at[i, c], buf.at[i, 1 - c], target(0, 0, 1))
            )
        first.append(arriving)
    exchange = {}

    def send_features(move):
        zz = moved(*move)
        arriving = []
        for flip in flips[1:]:
            px, py, pc = peer(*flip)
            other = px * shards + 2 * py + pc
            arriving.append(
                remote(
                    x_ref.at[:, features(zz, px, py, pc)], xin.at[zz, group_at],
                    xin.at[zz, other], target(*flip),
                )
            )
        exchange[move] = arriving


    prompt_len, chosen_len = len_ref[0, 0], len_ref[0, 1]
    reject_start = prompt_len + chosen_len
    key_row = lax.broadcasted_iota(jnp.int32, (seq, 1), 0)
    key_pos = stored_positions(key_row, rows, shards)
    chosen = jnp.logical_and(key_pos >= prompt_len, key_pos < reject_start)
    key_end = jnp.where(chosen, reject_start, 2 * seq)
    lane_row = lax.broadcasted_iota(jnp.int32, (1, head_cols), 1) % rows
    part_copies, out_copies = [], []
    for i in range(local_heads):
        per_head = own_count // local_heads
        for copy in own[i * per_head : (i + 1) * per_head]:
            copy.wait()
        for copy in first[i]:
            copy.wait_recv()
        if i == 0:
            send_features(moves[0])
            send_features(moves[1])
        keys = kbuf[i].reshape(seq, HEAD)
        values = vbuf[i].reshape(seq, HEAD)
        acc[...] = jnp.zeros_like(acc)

        def unit(a, carry):
            shard = 2 * y + a
            low = shard * half
            high = (2 * shards - 1 - shard) * half
            query_pos = jnp.where(lane_row >= half, high - half + lane_row, low + lane_row)
            starts = [h * HEAD for h in range(group)]
            queries = jnp.concatenate([qbuf[i, a, :, s : s + HEAD] for s in starts], axis=0)
            grads = jnp.concatenate([obuf[i, a, :, s : s + HEAD] for s in starts], axis=0)
            last = (((1,), (1,)), ((), ()))
            first_dims = (((0,), (0,)), ((), ()))
            scores = lax.dot_general(keys, queries, last, preferred_element_type=jnp.float32)
            prob_grad = lax.dot_general(values, grads, last, preferred_element_type=jnp.float32)
            allowed = jnp.logical_and(key_pos <= query_pos, query_pos < key_end)
            scores = jnp.where(allowed, scores, masked_fill)
            top = jnp.max(scores, axis=0, keepdims=True)
            weights = jnp.exp((scores - top) * scale)
            inverse = 1.0 / jnp.sum(weights, axis=0, keepdims=True)
            delta = jnp.sum(weights * prob_grad, axis=0, keepdims=True) * inverse
            probs = (weights * inverse).astype(jnp.bfloat16)
            score_grad = (weights * (prob_grad - delta) * (scale * inverse)).astype(jnp.bfloat16)
            acc[:, :HEAD] += jnp.dot(score_grad, queries, preferred_element_type=jnp.float32)
            acc[:, HEAD:] += jnp.dot(probs, grads, preferred_element_type=jnp.float32)
            query_grad = lax.dot_general(
                score_grad, keys, first_dims, preferred_element_type=jnp.float32
            ).astype(jnp.bfloat16)
            for h in range(group):
                dqbuf[i, a, :, h * HEAD : (h + 1) * HEAD] = query_grad[h * rows : (h + 1) * rows]
            return carry

        lax.fori_loop(0, 2, unit, 0)
        part[i] = acc[...].astype(jnp.bfloat16)
        part_copies.append(remote(part.at[i], precv.at[i], precv.at[i], target(0, 1, 0)))
        if i == 0:
            send_features(moves[2])
        if i == local_heads - 1:
            send_features(moves[3])
        own_cols = cols((c * local_heads + i) * head_cols, head_cols)
        other_cols = cols(((1 - c) * local_heads + i) * head_cols, head_cols)
        out_copies.append(
            remote(
                dqbuf.at[i, 1 - c], qg_ref.at[:, own_cols], qg_ref.at[:, other_cols], target(0, 0, 1)
            )
        )
        own.append(local(dqbuf.at[i, c], qg_ref.at[:, own_cols]))

    for copy in own_x:
        copy.wait()
    ready = set()

    def turn_features(move):
        if move in ready:
            return
        ready.add(move)
        zz = moved(*move)
        for copy in exchange[move]:
            copy.wait_recv()
        for at in range(2 * shards):
            xt[zz, :, at * rows : (at + 1) * rows] = xin[zz, at].T

    turn_features(moves[0])
    turn_features(moves[1])
    sibling = 2 * y + 1 - c
    to_x, to_sibling = [], []
    for i in range(local_heads):
        if i == local_heads - 1:
            turn_features(moves[2])
        part_copies[i].wait_recv()
        total = part[i].astype(jnp.float32) + precv[i].astype(jnp.float32)
        key_sum, value_sum = total[:, :HEAD], total[:, HEAD:]
        kgbuf[i] = key_sum.astype(jnp.bfloat16)
        g, other_g = c * local_heads + i, (1 - c) * local_heads + i
        turned = pltpu.roll(key_sum, HEAD // 2, 1)
        gbuf[g, x, :, :HEAD] = (key_sum * cos_ref[...] + turned * sin_ref[...]).astype(jnp.bfloat16)
        gbuf[g, x, :, HEAD:] = value_sum.astype(jnp.bfloat16)
        to_x.append(remote(gbuf.at[g, x], gbuf.at[g, x], gbuf.at[g, 1 - x], target(1, 0, 0)))
        to_sibling.append(
            remote(gbuf.at[g, x], gbuf.at[g, x], gbuf.at[other_g, x], target(0, 0, 1))
        )
        own_cols, other_cols = cols(g * HEAD, HEAD), cols(other_g * HEAD, HEAD)
        for buf, out in (
            (kgbuf.at[i], kg_ref),
            (gbuf.at[g, x, :, HEAD : 2 * HEAD], vg_ref),
        ):
            own.append(local(buf.at[rows_of(b), :], out.at[:, own_cols]))
            out_copies.append(
                remote(
                    buf.at[rows_of(sibling), :], out.at[:, own_cols], out.at[:, other_cols],
                    target(0, 0, 1),
                )
            )

    def z_target(move):
        return (2 * moved(*move) + x, b)

    crossed, direct = [], []
    turn_features(moves[3])
    for i in range(local_heads):
        g, other_g = c * local_heads + i, (1 - c) * local_heads + i
        to_x[i].wait_recv()
        relayed = remote(
            gbuf.at[g, 1 - x], gbuf.at[g, 1 - x], gbuf.at[other_g, 1 - x], target(0, 0, 1)
        )
        to_sibling[i].wait_recv()
        relayed.wait_recv()

        def product(move, j):
            grad_cols = gbuf[j * local_heads + i].reshape(2 * seq, 2 * HEAD)
            return jnp.dot(xt[moved(*move)], grad_cols, preferred_element_type=jnp.float32)

        halves = [slice(j * 2 * HEAD, (j + 1) * 2 * HEAD) for j in range(2)]
        for j in range(2):
            wbuf[i, 0, :, halves[j]] = product((1, 1), j).astype(jnp.bfloat16)
        before = remote(wbuf.at[i, 0], zrecv.at[i, 0], zrecv.at[i, 0], z_target((0, 1)))
        for j in range(2):
            wbuf[i, 1, :, halves[j]] = product((0, 1), j).astype(jnp.bfloat16)
        direct.append(remote(wbuf.at[i, 1], zrecv.at[i, 1], zrecv.at[i, 1], z_target((0, 1))))
        for j in range(2):
            wown[0, :, halves[j]] = product((1, 0), j)
        for j in range(2):
            wown[1 + i, :, halves[j]] = product((0, 0), j)
        before.wait_recv()
        wbuf[i, 2] = (wown[0] + zrecv[i, 0].astype(jnp.float32)).astype(jnp.bfloat16)
        crossed.append(remote(wbuf.at[i, 2], zrecv.at[i, 2], zrecv.at[i, 2], z_target((1, 0))))

    for i in range(local_heads):
        direct[i].wait_recv()
        crossed[i].wait_recv()
        total = (
            wown[1 + i] + zrecv[i, 1].astype(jnp.float32) + zrecv[i, 2].astype(jnp.float32)
        )
        for j in range(2):
            g = j * local_heads + i
            for kind in range(2):
                at = kind * kv_heads * HEAD + g * HEAD
                piece = (2 * j + kind) * HEAD
                w_ref[:, at : at + HEAD] = total[:, piece : piece + HEAD]
    for copy in own[own_count:]:
        copy.wait()
    for copy in out_copies:
        copy.wait_recv()
    for copy in pending:
        copy.wait_send()


def fused_body(queries, keys, values, out_grad, layer_input, lengths):
    shards = lax.axis_size("blk")
    depth = lax.axis_size("dp") // 2
    rows = queries.shape[1]
    kv_heads = keys.shape[2] // HEAD
    local_heads = kv_heads // 2
    group = queries.shape[2] // keys.shape[2]
    seq = rows * shards
    half_dim = HEAD // 2
    stored = np.arange(seq)
    block = stored // (rows // 2)
    holder = block // 2
    block = np.where(block % 2 == 1, 2 * shards - 1 - holder, holder)
    positions = (block * (rows // 2) + stored % (rows // 2)).astype(np.float32)
    frequency = np.exp(
        -(np.float32(2.0) * np.arange(half_dim, dtype=np.float32) / np.float32(HEAD))
        * np.float32(math.log(rope_base))
    ).astype(np.float32)
    angles = positions[:, None] * frequency[None, :]
    cosine = np.concatenate([np.cos(angles), np.cos(angles)], axis=1).astype(np.float32)
    sine = np.concatenate([np.sin(angles), -np.sin(angles)], axis=1).astype(np.float32)
    vmem = pl.BlockSpec(memory_space=pltpu.VMEM)
    anywhere = pl.BlockSpec(memory_space=pl.ANY)
    half = jnp.bfloat16
    remote_count = 8 * local_heads + 7 * depth + 2 * local_heads + 4 * local_heads + local_heads
    remote_count += 3 * local_heads
    local_count = 4 * local_heads + depth + 3 * local_heads
    features = layer_input.shape[2] // (2 * depth * shards)
    assert features == HEAD
    outs = pl.pallas_call(
        functools.partial(fused_kernel, (rows, local_heads, group, shards, depth)),
        out_shape=(
            jax.ShapeDtypeStruct(queries.shape[1:], half),
            jax.ShapeDtypeStruct(keys.shape[1:], half),
            jax.ShapeDtypeStruct(values.shape[1:], half),
            jax.ShapeDtypeStruct((features, 2 * kv_heads * HEAD), jnp.float32),
        ),
        in_specs=[pl.BlockSpec(memory_space=pltpu.SMEM)] + [anywhere] * 5 + [vmem] * 2,
        out_specs=(vmem,) * 4,
        scratch_shapes=[
            pltpu.VMEM((local_heads, 2, rows, group * HEAD), half),
            pltpu.VMEM((local_heads, 2, rows, group * HEAD), half),
            pltpu.VMEM((local_heads, shards, rows, HEAD), half),
            pltpu.VMEM((local_heads, shards, rows, HEAD), half),
            pltpu.VMEM((local_heads, 2, rows, group * HEAD), half),
            pltpu.VMEM((seq, 2 * HEAD), jnp.float32),
            pltpu.VMEM((local_heads, seq, 2 * HEAD), half),
            pltpu.VMEM((local_heads, seq, 2 * HEAD), half),
            pltpu.VMEM((local_heads, seq, HEAD), half),
            pltpu.VMEM((kv_heads, 2, seq, 2 * HEAD), half),
            pltpu.VMEM((depth, 2 * shards, rows, features), half),
            pltpu.VMEM((depth, features, 2 * seq), half),
            pltpu.VMEM((local_heads, 3, features, 4 * HEAD), half),
            pltpu.VMEM((local_heads, 3, features, 4 * HEAD), half),
            pltpu.VMEM((1 + local_heads, features, 4 * HEAD), jnp.float32),
            pltpu.SemaphoreType.DMA((local_count,)),
            pltpu.SemaphoreType.DMA((remote_count,)),
            pltpu.SemaphoreType.DMA((remote_count,)),
        ],
        compiler_params=pltpu.CompilerParams(
            collective_id=0, has_side_effects=True, vmem_limit_bytes=56 * 1024 * 1024
        ),
    )(
        lengths, queries[0], keys[0], values[0], out_grad[0], layer_input[0],
        jnp.asarray(cosine), jnp.asarray(sine),
    )
    query_grad, key_grad, value_grad, weight_grad = outs
    return (query_grad[None], key_grad[None], value_grad[None], weight_grad)


def chosen_body(queries, keys, values, out_grad, layer_input, lengths):
    shards, replicas = lax.axis_size("blk"), lax.axis_size("dp")
    paired = shards == 2 * 2 and replicas == 2 * shards
    kv_heads = keys.shape[2] // HEAD
    even = kv_heads % 2 == 0 and queries.shape[1] % HEAD == 0
    if paired and even and layer_input.shape[2] == replicas * shards * HEAD:
        return fused_body(queries, keys, values, out_grad, layer_input, lengths)
    return body(queries, keys, values, out_grad, layer_input, lengths)


def solution(mesh):
    placed = (
        P("dp", "blk", None),
        P("dp", "blk", None),
        P("dp", "blk", None),
        P("dp", "blk", None),
        P("dp", "blk", None),
        P("dp", None),
    )
    return jax.shard_map(
        chosen_body,
        mesh=mesh,
        in_specs=placed,
        out_specs=(
            P("dp", "blk", None),
            P("dp", "blk", None),
            P("dp", "blk", None),
            P(("dp", "blk"), None),
        ),
        check_vma=False,
    )
```

```python
import functools
import math

import jax
import jax.numpy as jnp
import numpy as np
from jax import lax
from jax.experimental import pallas as pl
from jax.experimental.pallas import tpu as pltpu
from jax.sharding import PartitionSpec as P

HEAD = 128


rope_base = 500000.0
masked_fill = -1e30


def stored_positions(stored_rows, shard_rows, shard_count):
    half_rows = shard_rows // 2
    block_number = stored_rows // half_rows
    holder = block_number // 2
    upper_half = block_number % 2
    position_block = jnp.where(upper_half == 1, 2 * shard_count - 1 - holder, holder)
    return (position_block * half_rows + stored_rows % half_rows).astype(jnp.int32)


def allowed_pairs(query_pos, key_pos, prompt_len, chosen_len):
    causal = key_pos[None, :] <= query_pos[:, None]
    reject_start = prompt_len + chosen_len
    query_rejected = query_pos >= reject_start
    key_chosen = jnp.logical_and(key_pos >= prompt_len, key_pos < reject_start)
    return jnp.logical_and(
        causal, jnp.logical_not(jnp.logical_and(query_rejected[:, None], key_chosen[None, :]))
    )


def block_length(total_rows):
    chosen_size = 1
    for candidate in range(1, min(total_rows, 512) + 1):
        if total_rows % candidate == 0:
            chosen_size = candidate
    return chosen_size


def over_blocks(running, pieces, first_row, block_fn):
    total_rows = pieces[0].shape[0]
    block_rows = block_length(total_rows)

    def one_turn(turn_index, current):
        block_start = turn_index * block_rows
        block_parts = tuple(
            (lax.dynamic_slice_in_dim(member, block_start, block_rows, 0) for member in pieces)
        )
        return block_fn(current, block_parts, first_row + block_start)

    return lax.fori_loop(0, total_rows // block_rows, one_turn, running)


def body(queries, keys, values, out_grad, layer_input, lengths):
    shard_count = lax.axis_size("blk")
    shard_index = lax.axis_index("blk")
    shard_rows = queries.shape[1]
    kv_heads = keys.shape[2] // HEAD
    group_heads = queries.shape[2] // keys.shape[2]
    seq_len = shard_rows * shard_count
    query_count = group_heads * shard_rows
    scale = 1.0 / math.sqrt(HEAD)
    prompt_len = lengths[0, 0]
    chosen_len = lengths[0, 1]
    own_rows = shard_index * shard_rows + jnp.arange(shard_rows, dtype=jnp.int32)
    own_pos = stored_positions(own_rows, shard_rows, shard_count)
    query_pos = jnp.tile(own_pos, group_heads)
    query_rows = (
        queries[0]
        .reshape(shard_rows, kv_heads, group_heads, HEAD)
        .transpose(1, 2, 0, 3)
        .reshape(kv_heads, query_count, HEAD)
    )
    grad_rows = (
        out_grad[0]
        .reshape(shard_rows, kv_heads, group_heads, HEAD)
        .transpose(1, 2, 0, 3)
        .reshape(kv_heads, query_count, HEAD)
    )

    def block_allowed(first_row, count_rows):
        key_pos = stored_positions(
            first_row + jnp.arange(count_rows, dtype=jnp.int32), shard_rows, shard_count
        )
        return allowed_pairs(query_pos, key_pos, prompt_len, chosen_len)

    def forward_block(running, block_parts, first_row):
        key_block, value_block = block_parts
        count_rows = key_block.shape[0]
        allowed = block_allowed(first_row, count_rows)
        run_max, run_sum, run_acc = running
        key_heads = key_block.reshape(count_rows, kv_heads, HEAD)
        value_heads = value_block.reshape(count_rows, kv_heads, HEAD).astype(jnp.float32)
        scores = scale * jnp.einsum(
            "gqe,kge->gqk", query_rows, key_heads, preferred_element_type=jnp.float32
        )
        new_max = jnp.maximum(
            run_max, jnp.max(jnp.where(allowed[None], scores, masked_fill), axis=-1)
        )
        weights = jnp.where(allowed[None], jnp.exp(scores - new_max[..., None]), 0.0)
        factor = jnp.exp(run_max - new_max)
        new_sum = run_sum * factor + jnp.sum(weights, axis=-1)
        new_acc = run_acc * factor[..., None] + jnp.einsum(
            "gqk,kge->gqe", weights, value_heads, precision=lax.Precision.HIGHEST
        )
        return (new_max, new_sum, new_acc)

    start_forward = (
        jnp.full((kv_heads, query_count), masked_fill, jnp.float32),
        jnp.zeros((kv_heads, query_count), jnp.float32),
        jnp.zeros((kv_heads, query_count, HEAD), jnp.float32),
    )
    run_max, run_sum, run_acc = over_blocks(
        start_forward,
        (
            lax.all_gather(keys[0], "blk", axis=0, tiled=True),
            lax.all_gather(values[0], "blk", axis=0, tiled=True),
        ),
        jnp.int32(0),
        forward_block,
    )
    attn_out = run_acc / run_sum[..., None]
    log_total = run_max + jnp.log(run_sum)
    delta = jnp.sum(grad_rows.astype(jnp.float32) * attn_out, axis=-1)

    def backward_block(running, block_parts, first_row):
        key_block, value_block = block_parts
        count_rows = key_block.shape[0]
        allowed = block_allowed(first_row, count_rows)
        query_acc, key_acc, value_acc = running
        key_heads = key_block.reshape(count_rows, kv_heads, HEAD)
        value_heads = value_block.reshape(count_rows, kv_heads, HEAD)
        scores = scale * jnp.einsum(
            "gqe,kge->gqk", query_rows, key_heads, preferred_element_type=jnp.float32
        )
        probs = jnp.where(allowed[None], jnp.exp(scores - log_total[..., None]), 0.0)
        prob_half = probs.astype(jnp.bfloat16)
        prob_grad = jnp.einsum(
            "gqe,kge->gqk", grad_rows, value_heads, preferred_element_type=jnp.float32
        )
        score_grad = (scale * probs * (prob_grad - delta[..., None])).astype(jnp.bfloat16)
        query_acc = query_acc + jnp.einsum(
            "gqk,kge->gqe", score_grad, key_heads, preferred_element_type=jnp.float32
        )
        key_term = jnp.einsum(
            "gqk,gqe->kge", score_grad, query_rows, preferred_element_type=jnp.float32
        ).reshape(count_rows, kv_heads * HEAD)
        value_term = jnp.einsum(
            "gqk,gqe->kge", prob_half, grad_rows, preferred_element_type=jnp.float32
        ).reshape(count_rows, kv_heads * HEAD)
        key_acc = lax.dynamic_update_slice_in_dim(
            key_acc,
            lax.dynamic_slice_in_dim(key_acc, first_row, count_rows, 0) + key_term,
            first_row,
            0,
        )
        value_acc = lax.dynamic_update_slice_in_dim(
            value_acc,
            lax.dynamic_slice_in_dim(value_acc, first_row, count_rows, 0) + value_term,
            first_row,
            0,
        )
        return (query_acc, key_acc, value_acc)

    start_backward = (
        jnp.zeros((kv_heads, query_count, HEAD), jnp.float32),
        jnp.zeros((seq_len, kv_heads * HEAD), jnp.float32),
        jnp.zeros((seq_len, kv_heads * HEAD), jnp.float32),
    )
    query_acc, key_acc, value_acc = over_blocks(
        start_backward,
        (
            lax.all_gather(keys[0], "blk", axis=0, tiled=True),
            lax.all_gather(values[0], "blk", axis=0, tiled=True),
        ),
        jnp.int32(0),
        backward_block,
    )
    key_sum, value_sum = (
        lax.psum_scatter(
            key_acc.astype(jnp.bfloat16), "blk", scatter_dimension=0, tiled=True
        ).astype(jnp.float32),
        lax.psum_scatter(
            value_acc.astype(jnp.bfloat16), "blk", scatter_dimension=0, tiled=True
        ).astype(jnp.float32),
    )
    query_grad = (
        query_acc.reshape(kv_heads, group_heads, shard_rows, HEAD)
        .transpose(2, 0, 1, 3)
        .reshape(shard_rows, kv_heads * group_heads * HEAD)
        .astype(jnp.bfloat16)
    )
    key_out = key_sum.astype(jnp.bfloat16)
    value_out = value_sum.astype(jnp.bfloat16)
    half_dim = HEAD // 2
    frequency = jnp.exp(
        -(2.0 * jnp.arange(half_dim, dtype=jnp.float32) / HEAD) * math.log(rope_base)
    )
    angles = own_pos.astype(jnp.float32)[:, None] * frequency[None, :]
    cosine = jnp.concatenate([jnp.cos(angles), jnp.cos(angles)], axis=-1)[:, None, :]
    sine = jnp.concatenate([jnp.sin(angles), jnp.sin(angles)], axis=-1)[:, None, :]
    grad_heads = key_sum.reshape(shard_rows, kv_heads, HEAD)
    rotated = jnp.concatenate([-grad_heads[..., half_dim:], grad_heads[..., :half_dim]], axis=-1)
    key_pre = (
        (grad_heads * cosine - rotated * sine)
        .reshape(shard_rows, kv_heads * HEAD)
        .astype(jnp.bfloat16)
    )
    grad_cols = jnp.concatenate([key_pre, value_out], axis=1)
    input_rows = layer_input[0]
    features = layer_input.shape[2]
    replica_count = lax.axis_size("dp")
    feature_share = features // (replica_count * shard_count)
    grouped_input = input_rows.reshape(shard_rows, replica_count, shard_count * feature_share)
    sequence_input = lax.all_to_all(grouped_input, "blk", split_axis=2, concat_axis=0, tiled=True)
    sequence_weight = jnp.einsum(
        "tif,tc->ifc",
        sequence_input,
        lax.all_gather(grad_cols, "blk", axis=0, tiled=True),
        preferred_element_type=jnp.float32,
    )
    weight_grad = (
        lax.psum_scatter(
            sequence_weight.astype(jnp.bfloat16), "dp", scatter_dimension=0, tiled=True
        )
        .astype(jnp.float32)
        .reshape(feature_share, grad_cols.shape[1])
    )
    return (query_grad[None], key_out[None], value_out[None], weight_grad)


def flipped(coordinate, bit):
    return 1 - coordinate if bit else coordinate


def fused_kernel(
    sizes, len_ref, q_ref, k_ref, v_ref, o_ref, x_ref, cos_ref, sin_ref,
    qg_ref, kg_ref, vg_ref, w_ref,
    qbuf, obuf, kbuf, vbuf, dqbuf, acc, part, precv, kgbuf, gbuf, xin, xt, wbuf, zrecv, wown,
    local_sem, send_sem, recv_sem,
):
    rows, local_heads, group, shards, depth = sizes
    seq = rows * shards
    half = rows // 2
    kv_heads = 2 * local_heads
    head_cols = group * HEAD
    scale = 1.0 / math.sqrt(HEAD)
    dp, b = lax.axis_index("dp"), lax.axis_index("blk")
    z, x = dp // 2, dp % 2
    y, c = b // 2, b % 2

    def peer(rx, ry, rc):
        px, py, pc = flipped(x, rx), flipped(y, ry), flipped(c, rc)
        return px, py, pc

    def target(rx, ry, rc):
        px, py, pc = peer(rx, ry, rc)
        return (2 * z + px, 2 * py + pc)

    counts = {"local": 0, "remote": 0}
    pending = []

    def local(src, dst):
        at = counts["local"]
        counts["local"] += 1
        copy = pltpu.make_async_copy(src, dst, local_sem.at[at])
        copy.start()
        return copy

    def remote(src, dst, landing, device):
        at = counts["remote"]
        counts["remote"] += 1
        copy = pltpu.make_async_remote_copy(
            src_ref=src, dst_ref=dst, send_sem=send_sem.at[at], recv_sem=recv_sem.at[at],
            device_id=device, device_id_type=pl.DeviceIdType.MESH,
        )
        copy.start()
        pending.append(copy)
        return pltpu.make_async_remote_copy(
            src_ref=src, dst_ref=landing, send_sem=send_sem.at[at], recv_sem=recv_sem.at[at],
            device_id=device, device_id_type=pl.DeviceIdType.MESH,
        )

    def cols(start, count):
        return pl.ds(pl.multiple_of(start, HEAD), count)

    def rows_of(shard):
        return pl.ds(pl.multiple_of(shard * rows, rows), rows)

    flips = [(rx, ry, rc) for rx in (0, 1) for ry in (0, 1) for rc in (0, 1)]
    barrier = pltpu.get_barrier_semaphore()
    for flip in flips[1:]:
        pl.semaphore_signal(
            barrier, inc=1, device_id=target(*flip), device_id_type=pl.DeviceIdType.MESH
        )
    moves = [(1, 1), (0, 1), (1, 0), (0, 0)]

    def moved(outer, inner):
        return 2 * flipped(z // 2, outer) + flipped(z % 2, inner)

    for move in moves[:-1]:
        pl.semaphore_signal(
            barrier, inc=1, device_id=(2 * moved(*move) + x, b),
            device_id_type=pl.DeviceIdType.MESH,
        )
    own = []
    for i in range(local_heads):
        at = c * local_heads + i
        own.append(local(k_ref.at[:, cols(at * HEAD, HEAD)], kbuf.at[i, b]))
        own.append(local(v_ref.at[:, cols(at * HEAD, HEAD)], vbuf.at[i, b]))
        own.append(local(q_ref.at[:, cols(at * head_cols, head_cols)], qbuf.at[i, c]))
        own.append(local(o_ref.at[:, cols(at * head_cols, head_cols)], obuf.at[i, c]))
    own_count = len(own)
    group_at = x * shards + b

    def features(zz, px, py, pc):
        return cols(((2 * zz + px) * shards + 2 * py + pc) * HEAD, HEAD)

    own_x = [
        local(x_ref.at[:, features(zz, x, y, c)], xin.at[zz, group_at]) for zz in range(depth)
    ]
    pl.semaphore_wait(barrier, len(flips) - 1 + len(moves) - 1)

    first = []
    for i in range(local_heads):
        arriving = []
        for flip in ((0, 1, 0), (0, 1, 1), (0, 0, 1)):
            _, py, pc = peer(*flip)
            other = 2 * py + pc
            columns = cols((pc * local_heads + i) * HEAD, HEAD)
            for ref, buf in ((k_ref, kbuf), (v_ref, vbuf)):
                arriving.append(
                    remote(ref.at[:, columns], buf.at[i, b], buf.at[i, other], target(*flip))
                )
        columns = cols(((1 - c) * local_heads + i) * head_cols, head_cols)
        for ref, buf in ((q_ref, qbuf), (o_ref, obuf)):
            arriving.append(
                remote(ref.at[:, columns], buf.at[i, c], buf.at[i, 1 - c], target(0, 0, 1))
            )
        first.append(arriving)
    exchange = {}

    def send_features(move):
        zz = moved(*move)
        arriving = []
        for flip in flips[1:]:
            px, py, pc = peer(*flip)
            other = px * shards + 2 * py + pc
            arriving.append(
                remote(
                    x_ref.at[:, features(zz, px, py, pc)], xin.at[zz, group_at],
                    xin.at[zz, other], target(*flip),
                )
            )
        exchange[move] = arriving


    prompt_len, chosen_len = len_ref[0, 0], len_ref[0, 1]
    reject_start = prompt_len + chosen_len
    key_row = lax.broadcasted_iota(jnp.int32, (seq, 1), 0)
    key_pos = stored_positions(key_row, rows, shards)
    chosen = jnp.logical_and(key_pos >= prompt_len, key_pos < reject_start)
    key_end = jnp.where(chosen, reject_start, 2 * seq)
    lane_row = lax.broadcasted_iota(jnp.int32, (1, head_cols), 1) % rows
    part_copies, out_copies = [], []
    for i in range(local_heads):
        per_head = own_count // local_heads
        for copy in own[i * per_head : (i + 1) * per_head]:
            copy.wait()
        for copy in first[i]:
            copy.wait_recv()
        keys = kbuf[i].reshape(seq, HEAD)
        values = vbuf[i].reshape(seq, HEAD)
        acc[...] = jnp.zeros_like(acc)

        def unit(a, carry):
            shard = 2 * y + a
            low = shard * half
            high = (2 * shards - 1 - shard) * half
            query_pos = jnp.where(lane_row >= half, high - half + lane_row, low + lane_row)
            starts = [h * HEAD for h in range(group)]
            queries = jnp.concatenate([qbuf[i, a, :, s : s + HEAD] for s in starts], axis=0)
            grads = jnp.concatenate([obuf[i, a, :, s : s + HEAD] for s in starts], axis=0)
            last = (((1,), (1,)), ((), ()))
            first_dims = (((0,), (0,)), ((), ()))
            scores = lax.dot_general(keys, queries, last, preferred_element_type=jnp.float32)
            prob_grad = lax.dot_general(values, grads, last, preferred_element_type=jnp.float32)
            allowed = jnp.logical_and(key_pos <= query_pos, query_pos < key_end)
            scores = jnp.where(allowed, scores, masked_fill)
            top = jnp.max(scores, axis=0, keepdims=True)
            weights = jnp.exp((scores - top) * scale)
            inverse = 1.0 / jnp.sum(weights, axis=0, keepdims=True)
            delta = jnp.sum(weights * prob_grad, axis=0, keepdims=True) * inverse
            probs = (weights * inverse).astype(jnp.bfloat16)
            score_grad = (weights * (prob_grad - delta) * (scale * inverse)).astype(jnp.bfloat16)
            acc[:, :HEAD] += jnp.dot(score_grad, queries, preferred_element_type=jnp.float32)
            acc[:, HEAD:] += jnp.dot(probs, grads, preferred_element_type=jnp.float32)
            query_grad = lax.dot_general(
                score_grad, keys, first_dims, preferred_element_type=jnp.float32
            ).astype(jnp.bfloat16)
            for h in range(group):
                dqbuf[i, a, :, h * HEAD : (h + 1) * HEAD] = query_grad[h * rows : (h + 1) * rows]
            return carry

        lax.fori_loop(0, 2, unit, 0)
        for kind in range(2):
            part[i, kind] = acc[:, kind * HEAD : (kind + 1) * HEAD].astype(jnp.bfloat16)
            part_copies.append(
                remote(part.at[i, kind], precv.at[i, kind], precv.at[i, kind], target(0, 1, 0))
            )
        if i == 0:
            send_features(moves[0])
            send_features(moves[1])
        own_cols = cols((c * local_heads + i) * head_cols, head_cols)
        other_cols = cols(((1 - c) * local_heads + i) * head_cols, head_cols)
        out_copies.append(
            remote(
                dqbuf.at[i, 1 - c], qg_ref.at[:, own_cols], qg_ref.at[:, other_cols], target(0, 0, 1)
            )
        )
        own.append(local(dqbuf.at[i, c], qg_ref.at[:, own_cols]))

    for copy in own_x:
        copy.wait()

    def turn_features(move):
        zz = moved(*move)
        for copy in exchange[move]:
            copy.wait_recv()
        for at in range(2 * shards):
            xt[zz, :, at * rows : (at + 1) * rows] = xin[zz, at].T

    sibling = 2 * y + 1 - c
    pieces = [(i, kind) for i in range(local_heads) for kind in range(2)]
    to_x, to_sibling = [], []
    for at, (i, kind) in enumerate(pieces):
        part_copies[at].wait_recv()
        total = part[i, kind].astype(jnp.float32) + precv[i, kind].astype(jnp.float32)
        g, other_g = c * local_heads + i, (1 - c) * local_heads + i
        mine = gbuf.at[kind, g, x]
        if kind == 0:
            kgbuf[i] = total.astype(jnp.bfloat16)
            turned = pltpu.roll(total, HEAD // 2, 1)
            gbuf[kind, g, x] = (total * cos_ref[...] + turned * sin_ref[...]).astype(jnp.bfloat16)
        else:
            gbuf[kind, g, x] = total.astype(jnp.bfloat16)
        to_x.append(remote(mine, mine, gbuf.at[kind, g, 1 - x], target(1, 0, 0)))
        to_sibling.append(remote(mine, mine, gbuf.at[kind, other_g, x], target(0, 0, 1)))
        own_cols, other_cols = cols(g * HEAD, HEAD), cols(other_g * HEAD, HEAD)
        buf, out = (kgbuf.at[i], kg_ref) if kind == 0 else (mine, vg_ref)
        own.append(local(buf.at[rows_of(b), :], out.at[:, own_cols]))
        out_copies.append(
            remote(
                buf.at[rows_of(sibling), :], out.at[:, own_cols], out.at[:, other_cols],
                target(0, 0, 1),
            )
        )
        if at == 0:
            send_features(moves[2])
            turn_features(moves[0])
            turn_features(moves[1])
        if at == 1:
            send_features(moves[3])

    def z_target(move):
        return (2 * moved(*move) + x, b)

    before, direct, crossed = [], [], []

    def cross(at):
        before[at].wait_recv()
        wbuf[at, 2] = (wown[at, 0] + zrecv[at, 0].astype(jnp.float32)).astype(jnp.bfloat16)
        crossed.append(remote(wbuf.at[at, 2], zrecv.at[at, 2], zrecv.at[at, 2], z_target((1, 0))))

    for at, (i, kind) in enumerate(pieces):
        g, other_g = c * local_heads + i, (1 - c) * local_heads + i
        to_x[at].wait_recv()
        theirs = gbuf.at[kind, g, 1 - x]
        relayed = remote(theirs, theirs, gbuf.at[kind, other_g, 1 - x], target(0, 0, 1))
        to_sibling[at].wait_recv()
        relayed.wait_recv()
        grad_cols = jnp.concatenate(
            [gbuf[kind, j * local_heads + i].reshape(2 * seq, HEAD) for j in range(2)], axis=1
        )

        def product(move):
            return jnp.dot(xt[moved(*move)], grad_cols, preferred_element_type=jnp.float32)

        wbuf[at, 0] = product((1, 1)).astype(jnp.bfloat16)
        before.append(remote(wbuf.at[at, 0], zrecv.at[at, 0], zrecv.at[at, 0], z_target((0, 1))))
        wbuf[at, 1] = product((0, 1)).astype(jnp.bfloat16)
        direct.append(remote(wbuf.at[at, 1], zrecv.at[at, 1], zrecv.at[at, 1], z_target((0, 1))))
        if at == 0:
            turn_features(moves[2])
        wown[at, 0] = product((1, 0))
        if at > 0:
            cross(at - 1)
        if at == 0:
            turn_features(moves[3])
        wown[at, 1] = product((0, 0))
    cross(len(pieces) - 1)

    for at, (i, kind) in enumerate(pieces):
        direct[at].wait_recv()
        crossed[at].wait_recv()
        total = wown[at, 1] + zrecv[at, 1].astype(jnp.float32) + zrecv[at, 2].astype(jnp.float32)
        for j in range(2):
            start = (kind * kv_heads + j * local_heads + i) * HEAD
            w_ref[:, start : start + HEAD] = total[:, j * HEAD : (j + 1) * HEAD]
    for copy in own[own_count:]:
        copy.wait()
    for copy in out_copies:
        copy.wait_recv()
    for copy in pending:
        copy.wait_send()


def fused_body(queries, keys, values, out_grad, layer_input, lengths):
    shards = lax.axis_size("blk")
    depth = lax.axis_size("dp") // 2
    rows = queries.shape[1]
    kv_heads = keys.shape[2] // HEAD
    local_heads = kv_heads // 2
    group = queries.shape[2] // keys.shape[2]
    seq = rows * shards
    half_dim = HEAD // 2
    stored = np.arange(seq)
    block = stored // (rows // 2)
    holder = block // 2
    block = np.where(block % 2 == 1, 2 * shards - 1 - holder, holder)
    positions = (block * (rows // 2) + stored % (rows // 2)).astype(np.float32)
    frequency = np.exp(
        -(np.float32(2.0) * np.arange(half_dim, dtype=np.float32) / np.float32(HEAD))
        * np.float32(math.log(rope_base))
    ).astype(np.float32)
    angles = positions[:, None] * frequency[None, :]
    cosine = np.concatenate([np.cos(angles), np.cos(angles)], axis=1).astype(np.float32)
    sine = np.concatenate([np.sin(angles), -np.sin(angles)], axis=1).astype(np.float32)
    vmem = pl.BlockSpec(memory_space=pltpu.VMEM)
    anywhere = pl.BlockSpec(memory_space=pl.ANY)
    half = jnp.bfloat16
    remote_count = 7 * depth + 25 * local_heads
    local_count = depth + 7 * local_heads
    features = layer_input.shape[2] // (2 * depth * shards)
    assert features == HEAD
    outs = pl.pallas_call(
        functools.partial(fused_kernel, (rows, local_heads, group, shards, depth)),
        out_shape=(
            jax.ShapeDtypeStruct(queries.shape[1:], half),
            jax.ShapeDtypeStruct(keys.shape[1:], half),
            jax.ShapeDtypeStruct(values.shape[1:], half),
            jax.ShapeDtypeStruct((features, 2 * kv_heads * HEAD), jnp.float32),
        ),
        in_specs=[pl.BlockSpec(memory_space=pltpu.SMEM)] + [anywhere] * 5 + [vmem] * 2,
        out_specs=(vmem,) * 4,
        scratch_shapes=[
            pltpu.VMEM((local_heads, 2, rows, group * HEAD), half),
            pltpu.VMEM((local_heads, 2, rows, group * HEAD), half),
            pltpu.VMEM((local_heads, shards, rows, HEAD), half),
            pltpu.VMEM((local_heads, shards, rows, HEAD), half),
            pltpu.VMEM((local_heads, 2, rows, group * HEAD), half),
            pltpu.VMEM((seq, 2 * HEAD), jnp.float32),
            pltpu.VMEM((local_heads, 2, seq, HEAD), half),
            pltpu.VMEM((local_heads, 2, seq, HEAD), half),
            pltpu.VMEM((local_heads, seq, HEAD), half),
            pltpu.VMEM((2, kv_heads, 2, seq, HEAD), half),
            pltpu.VMEM((depth, 2 * shards, rows, features), half),
            pltpu.VMEM((depth, features, 2 * seq), half),
            pltpu.VMEM((2 * local_heads, 3, features, 2 * HEAD), half),
            pltpu.VMEM((2 * local_heads, 3, features, 2 * HEAD), half),
            pltpu.VMEM((2 * local_heads, 2, features, 2 * HEAD), jnp.float32),
            pltpu.SemaphoreType.DMA((local_count,)),
            pltpu.SemaphoreType.DMA((remote_count,)),
            pltpu.SemaphoreType.DMA((remote_count,)),
        ],
        compiler_params=pltpu.CompilerParams(
            collective_id=0, has_side_effects=True, vmem_limit_bytes=56 * 1024 * 1024
        ),
    )(
        lengths, queries[0], keys[0], values[0], out_grad[0], layer_input[0],
        jnp.asarray(cosine), jnp.asarray(sine),
    )
    query_grad, key_grad, value_grad, weight_grad = outs
    return (query_grad[None], key_grad[None], value_grad[None], weight_grad)


def chosen_body(queries, keys, values, out_grad, layer_input, lengths):
    shards, replicas = lax.axis_size("blk"), lax.axis_size("dp")
    paired = shards == 2 * 2 and replicas == 2 * shards
    kv_heads = keys.shape[2] // HEAD
    even = kv_heads % 2 == 0 and queries.shape[1] % HEAD == 0
    if paired and even and layer_input.shape[2] == replicas * shards * HEAD:
        return fused_body(queries, keys, values, out_grad, layer_input, lengths)
    return body(queries, keys, values, out_grad, layer_input, lengths)


def solution(mesh):
    placed = (
        P("dp", "blk", None),
        P("dp", "blk", None),
        P("dp", "blk", None),
        P("dp", "blk", None),
        P("dp", "blk", None),
        P("dp", None),
    )
    return jax.shard_map(
        chosen_body,
        mesh=mesh,
        in_specs=placed,
        out_specs=(
            P("dp", "blk", None),
            P("dp", "blk", None),
            P("dp", "blk", None),
            P(("dp", "blk"), None),
        ),
        check_vma=False,
    )
```
